32 devices in a mesh: expert: 8 (over y, x, core), dp: 4 (over z).
Axes of the slice: x: 2, y: 2, z: 4, core: 2. Of those that a mesh axis runs over, the one named last changes fastest.
Arguments:
- patches: bfloat16 [8192, 1024], P(('expert', 'dp')), may hold values from -6 to 6
- router_weight: bfloat16 [1024, 8], replicated, may hold values from -0.1875 to 0.1875
- router_bias: float32 [8], replicated, may hold values from -1.5 to 1.5
- noise: float32 [8192, 8], P(('expert', 'dp')), may hold values from -5 to 5
- top_experts: int32 [8192, 2], P(('expert', 'dp')), may hold values from 0 to 7, all different within a row; in each aligned block of 256 rows (0 to 255, 256 to 511, ...) at most 80 rows name the same one
- threshold_expert: int32 [8192], P(('expert', 'dp')), may hold values from 0 to 7
- w_in: bfloat16 [8, 1024, 2048], P('expert'), may hold values from -0.1875 to 0.1875
- w_out: bfloat16 [8, 2048, 1024], P('expert'), may hold values from -0.125 to 0.125
- out_grad: bfloat16 [8192, 1024], P(('expert', 'dp')), may hold values from -24 to 24
Outputs:
- patch_grad: bfloat16 [8192, 1024], P(('expert', 'dp'))
- w_in_grad: bfloat16 [8, 1024, 2048], P('expert', None, 'dp')
- w_out_grad: bfloat16 [8, 2048, 1024], P('expert', 'dp')
- router_weight_grad: float32 [1024, 8], replicated
- router_bias_grad: float32 [8], replicated
The draws below stay inside these ranges and needn't reach their ends.
Inputs may be any that keep to these rules, and one draw needn't show every extreme that they name: `top_experts`: the two experts of a patch differ; among the patches of one device no expert is named more than 80 times.
All inputs are finite; a program needn't handle non-finite values.
Results may differ from the reference program's by a relative error of at most 0.0062.
The reference program's roundings to bfloat16 on the way (of `gates`, `hidden_grad`, `rows_back` and `logit_low`) count: a program that leaves them out, or rounds other values in their place, can miss the bound.
Values may be sent and summed in bfloat16 or wider, within the bound.
A program may use at most 128 MiB of HBM per device.

```python
import math
import jax
import jax.numpy as jnp
import numpy as np
from jax import lax

D = 1024
FFW = 2048
TOK_DEV = 256
E = 8
CAP = 80
TOKENS = 8192


def place_ends(result, own_key, least, largest):
    dims = result.shape
    index_at = [jax.random.randint(jax.random.fold_in(own_key, axis), (), 0, dims[axis]) for axis in range(len(dims))]
    result = result.at[tuple(index_at)].set(least)
    longest = dims.index(max(dims))
    index_at[longest] = (index_at[longest] + 1) % dims[longest]
    return result.at[tuple(index_at)].set(largest)


def level_of(rng, shape, shards, low, high):
    loudness, own = 1.0, jax.random.fold_in(rng, 6)
    for position, shards_of in shards:
        heights = jnp.exp(jax.random.uniform(jax.random.fold_in(own, position), (shards_of,), jnp.float32, low / len(shards), high / len(shards)))
        loudness = loudness * jnp.repeat(heights, shape[position] // shards_of).reshape([-1 if axis == position else 1 for axis in range(len(shape))])
    return loudness


def shared_out(key, own, number, rows, count, top, most, skew):
    order = jax.random.permutation(key, count)
    heavy_load, common = load_shares(count, rows * top, most, skew, True), load_shares(count, rows * top, most, skew, False)
    places = jnp.arange(count)

    def named(sizes, offset_by):
        used = int((sizes > 0).sum())
        fixed = max(1, used // 4)
        moved = fixed + (places - fixed + offset_by * (used - fixed)) % max(1, count - fixed)
        return jnp.zeros((count,), jnp.int32).at[order[jnp.where(places < fixed, places, moved)]].set(jnp.asarray(sizes, jnp.int32))

    sizes = jnp.where(number % 4 == 0, named(heavy_load, number // 4), named(common, number - number // 4 - 1))
    mixed = jax.random.permutation(jax.random.fold_in(own, 3), count)
    donor, taker = mixed[0:count // 2 * 2:2], mixed[1:count // 2 * 2:2]
    slack = jnp.minimum(sizes[donor] - 1, most - sizes[taker]) // 2
    slack = jnp.where((donor == order[0]) | (taker == order[0]) | (sizes[taker] == 0), 0, jnp.maximum(slack, 0))
    moved = jax.random.randint(jax.random.fold_in(own, 4), (count // 2,), 0, 1 << 20) % (slack + 1)
    sizes = sizes.at[donor].add(-moved).at[taker].add(moved)
    members = jnp.searchsorted(jnp.cumsum(sizes), jnp.arange(rows * top), side="right").astype(jnp.int32)
    table = members.reshape(top, rows).T
    table = table[jax.random.permutation(jax.random.fold_in(own, 1), rows)]
    offset_by = jax.random.randint(jax.random.fold_in(own, 2), (rows, 1), 0, top)
    return jnp.take_along_axis(table, (jnp.arange(top)[None, :] + offset_by) % top, axis=1)


def load_shares(count, total, bound, skew, full):
    portions = [(1 << 20) // math.isqrt(grade ** skew) + 1 for grade in range(1, count + 1)]
    largest = bound if full else min(bound, max(-(-total // count), total * portions[0] // sum(portions)))
    least = 1 if total - largest >= count - 1 else 0
    counts, rest = [largest] + [least] * (count - 1), total - largest - least * (count - 1)
    while rest > 0:
        candidates = [i for i in range(1, count) if counts[i] < largest] or [i for i in range(1, count) if counts[i] < bound]
        mass, left = sum([portions[i] for i in candidates]), rest
        for i in candidates:
            addition = min(bound - counts[i], max(1, left * portions[i] // mass), rest)
            counts[i] = counts[i] + addition
            rest = rest - addition
    return np.array(counts)


def scatter_about(key, shape, deviation, limit, pieces=(), kind=jnp.bfloat16):
    drawn = deviation * jax.random.normal(key, shape, jnp.float32)
    if pieces:
        drawn = drawn * level_of(key, shape, pieces, -0.22, 0.18)
    return jnp.clip(drawn, -limit, limit).astype(kind)


def setup_inputs(seed: int = 0) -> dict:
    key_of = jax.random.split(jax.random.key(seed), 10)
    patches = scatter_about(key_of[0], (TOKENS, D), 1.0, 6.0, ((0, 32),))
    router_weight = scatter_about(key_of[1], (D, E), D ** -0.5, 0.1875)
    router_bias = jnp.clip(jax.random.uniform(key_of[2], (E,), jnp.float32, -1.5, 1.5), -1.5, 1.5)
    noise = scatter_about(key_of[3], (TOKENS, E), 1.0, 5.0, ((0, 32),), jnp.float32)
    top_experts_keys = jax.random.split(jax.random.fold_in(key_of[4], 1), TOKENS // TOK_DEV)
    top_experts_turns = jax.random.permutation(jax.random.fold_in(key_of[4], 3), TOKENS // TOK_DEV)
    top_experts = jax.vmap(lambda own, number: shared_out(jax.random.fold_in(key_of[4], 2), own, number, TOK_DEV, E, 2, CAP, 1))(top_experts_keys, top_experts_turns).reshape((TOKENS, 2))
    threshold_expert = place_ends(jax.random.randint(key_of[5], (TOKENS,), 0, E), jax.random.fold_in(key_of[5], 1), 0, E - 1).astype(jnp.int32)
    w_in = scatter_about(key_of[6], (E, D, FFW), D ** -0.5, 0.1875, ((0, 8),))
    w_out = scatter_about(key_of[7], (E, FFW, D), FFW ** -0.5, 0.125, ((0, 8),))
    out_grad = scatter_about(key_of[8], (TOKENS, D), 4.0, 24.0, ((0, 32),))
    return dict(patches=patches, router_weight=router_weight, router_bias=router_bias, noise=noise, top_experts=top_experts, threshold_expert=threshold_expert, w_in=w_in, w_out=w_out, out_grad=out_grad)


noise_std = 1.0
aux_weight = 1.0
inv_root_two = 0.7071067811865476
inv_root_tau = 0.3989422804014327

def gelu_tanh(values):
    return jax.nn.gelu(values, approximate=True)

def spread_grad(values):
    number = values.shape[0]
    average = jnp.mean(values)
    spread = jnp.mean((values - average) ** 2)
    return (2.0 * (values - average) - 2.0 * spread / average) / (number * average * average)

def expert_terms(rows_in, rows_grad, rows_gate, w_first, w_second):
    hidden = jnp.dot(rows_in, w_first, preferred_element_type=jnp.float32)
    active, pullback = jax.vjp(gelu_tanh, hidden)
    active_low = lax.optimization_barrier(active.astype(jnp.bfloat16))
    back_proj = jnp.dot(rows_grad, w_second.T, preferred_element_type=jnp.float32)
    gate_col = rows_gate.astype(jnp.float32)[:, None]
    gate_terms = lax.optimization_barrier(jnp.sum(back_proj * active_low.astype(jnp.float32), axis=-1))
    hidden_grad = pullback(gate_col * back_proj)[0].astype(jnp.bfloat16)
    scaled_grad = (gate_col * rows_grad.astype(jnp.float32)).astype(jnp.bfloat16)
    first_grad = jnp.dot(rows_in.T, hidden_grad, preferred_element_type=jnp.float32)
    second_grad = jnp.dot(active_low.T, scaled_grad, preferred_element_type=jnp.float32)
    rows_back = jnp.dot(hidden_grad, w_first.T, preferred_element_type=jnp.float32)
    return (first_grad, second_grad, rows_back, gate_terms)

def reference(patches, router_weight, router_bias, noise, top_experts, threshold_expert, w_in, w_out, out_grad):
    tokens = patches.shape[0]
    width = patches.shape[1]
    experts = router_weight.shape[1]
    blocks = tokens // TOK_DEV
    logits = jnp.dot(patches, router_weight, preferred_element_type=jnp.float32) + router_bias
    noisy = logits + noise_std * noise
    probs = jax.nn.softmax(noisy, axis=-1)
    expert_ids = lax.broadcasted_iota(jnp.int32, (1, experts), 1)
    thresh_hot = threshold_expert[:, None] == expert_ids
    base = lax.optimization_barrier(jnp.sum(jnp.where(thresh_hot, noisy, 0.0), axis=-1, keepdims=True))
    zscore = (logits - base) / noise_std
    importance = lax.optimization_barrier(jnp.sum(probs, axis=0))
    load = lax.optimization_barrier(jnp.sum(0.5 * (1.0 + lax.erf(zscore * inv_root_two)), axis=0))
    top_hot = top_experts[:, :, None] == expert_ids[None]
    gates = lax.optimization_barrier(jnp.sum(jnp.where(top_hot, probs[:, None, :], 0.0), axis=-1)).astype(jnp.bfloat16)
    flat = top_experts.reshape(blocks, 2 * TOK_DEV)
    flat_hot = (flat[:, :, None] == expert_ids[None]).astype(jnp.int32)
    before = lax.optimization_barrier(jnp.sum((jnp.cumsum(flat_hot, axis=1) - flat_hot) * flat_hot, axis=-1)).astype(jnp.int32)
    slot_rows = (jnp.arange(blocks, dtype=jnp.int32)[:, None] * CAP + before).astype(jnp.int32)
    token_ids = (jnp.arange(2 * tokens, dtype=jnp.int32) // 2).reshape(blocks, 2 * TOK_DEV)
    table = jnp.full((experts, blocks * CAP), tokens, jnp.int32).at[flat, slot_rows].set(token_ids)
    gate_table = jnp.zeros((experts, blocks * CAP), jnp.bfloat16).at[flat, slot_rows].set(gates.reshape(blocks, 2 * TOK_DEV))

    def one_expert(operands):
        w_first, w_second, index_row, gate_row = operands
        valid = (index_row < tokens)[:, None]
        safe = jnp.minimum(index_row, tokens - 1)
        rows_in = jnp.where(valid, patches[safe], jnp.zeros((), jnp.bfloat16))
        rows_grad = jnp.where(valid, out_grad[safe], jnp.zeros((), jnp.bfloat16))
        first_grad, second_grad, rows_back, gate_terms = expert_terms(rows_in, rows_grad, gate_row, w_first, w_second)
        return (first_grad.astype(jnp.bfloat16), second_grad.astype(jnp.bfloat16), rows_back.astype(jnp.bfloat16), gate_terms.astype(jnp.bfloat16))
    first_all, second_all, back_all, gate_all = lax.map(one_expert, (w_in, w_out, table, gate_table))
    picked = back_all[flat, slot_rows].astype(jnp.float32).reshape(tokens, 2, width)
    expert_back = lax.optimization_barrier(jnp.sum(picked, axis=1))
    gate_grad = gate_all[flat, slot_rows].astype(jnp.float32).reshape(tokens, 2)
    total_weight = aux_weight * tokens
    imp_coef = total_weight * spread_grad(importance)
    load_coef = total_weight * spread_grad(load)
    score_grad = lax.optimization_barrier(jnp.sum(jnp.where(top_hot, gate_grad[:, :, None], 0.0), axis=1)) + imp_coef[None, :]
    noisy_grad = probs * (score_grad - lax.optimization_barrier(jnp.sum(probs * score_grad, axis=-1, keepdims=True)))
    z_grad = load_coef[None, :] * inv_root_tau * jnp.exp(-0.5 * zscore * zscore)
    logit_grad = noisy_grad + z_grad / noise_std - jnp.where(thresh_hot, lax.optimization_barrier(jnp.sum(z_grad, axis=-1, keepdims=True)) / noise_std, 0.0)
    logit_low = logit_grad.astype(jnp.bfloat16)
    router_back = jnp.dot(logit_low, router_weight.T, preferred_element_type=jnp.float32)
    patch_grad = (expert_back + router_back).astype(jnp.bfloat16)
    router_weight_grad = jnp.dot(patches.T, logit_low, preferred_element_type=jnp.float32)
    router_bias_grad = lax.optimization_barrier(jnp.sum(logit_grad, axis=0))
    return (patch_grad, first_all, second_all, router_weight_grad, router_bias_grad)
```

```python
import jax
import jax.numpy as jnp
from jax import lax
from jax.sharding import PartitionSpec as P


noise_std = 1.0
aux_weight = 1.0
inv_root_two = 0.7071067811865476
inv_root_tau = 0.3989422804014327


def gelu_tanh(values):
    return jax.nn.gelu(values, approximate=True)


def spread_grad(values):
    number = values.shape[0]
    average = jnp.mean(values)
    spread = jnp.mean((values - average) ** 2)
    return (2.0 * (values - average) - 2.0 * spread / average) / (number * average * average)


def on_device(
    patches, router_weight, router_bias, noise, top_experts, threshold_expert, w_in, w_out, out_grad
):
    tok_rows = patches.shape[0]
    width = patches.shape[1]
    experts = router_weight.shape[1]
    capacity = 5 * tok_rows // (2 * experts)
    slots = experts * capacity
    total_tokens = tok_rows * lax.axis_size("expert") * lax.axis_size("dp")
    logits = jnp.dot(patches, router_weight, preferred_element_type=jnp.float32) + router_bias
    noisy = logits + noise_std * noise
    probs = jax.nn.softmax(noisy, axis=-1)
    expert_ids = lax.broadcasted_iota(jnp.int32, (1, experts), 1)
    thresh_hot = threshold_expert[:, None] == expert_ids
    base = jnp.sum(jnp.where(thresh_hot, noisy, 0.0), axis=-1, keepdims=True)
    zscore = (logits - base) / noise_std
    stat_sums = (
        jnp.sum(probs, axis=0),
        jnp.sum(0.5 * (1.0 + lax.erf(zscore * inv_root_two)), axis=0),
    )
    top_hot = top_experts[:, :, None] == expert_ids[None]
    gates = jnp.sum(jnp.where(top_hot, probs[:, None, :], 0.0), axis=-1).astype(jnp.bfloat16)
    flat = top_experts.reshape(-1)
    flat_hot = (flat[:, None] == expert_ids).astype(jnp.int32)
    before = jnp.sum((jnp.cumsum(flat_hot, axis=0) - flat_hot) * flat_hot, axis=-1)
    slot_ids = flat * capacity + before
    slot_index = lax.broadcasted_iota(jnp.int32, (slots, 1), 0)
    assign = (slot_index == slot_ids[None, :]).astype(jnp.bfloat16)
    assign_tok = jnp.sum(assign.reshape(slots, tok_rows, 2), axis=-1)
    sent_in = (
        jnp.dot(assign_tok, patches, preferred_element_type=jnp.float32)
        .astype(jnp.bfloat16)
        .reshape(experts, capacity, width)
    )
    sent_grad = (
        jnp.dot(assign_tok, out_grad, preferred_element_type=jnp.float32)
        .astype(jnp.bfloat16)
        .reshape(experts, capacity, width)
    )
    sent_gate = (
        jnp.dot(assign, gates.reshape(-1), preferred_element_type=jnp.float32)
        .astype(jnp.bfloat16)
        .reshape(experts, capacity)
    )
    recv_in, recv_grad, recv_gate = (
        lax.all_to_all(sent_in, "expert", split_axis=0, concat_axis=0, tiled=True),
        lax.all_to_all(sent_grad, "expert", split_axis=0, concat_axis=0, tiled=True),
        lax.all_to_all(sent_gate, "expert", split_axis=0, concat_axis=0, tiled=True),
    )
    rows_in = recv_in.reshape(slots, width)
    rows_grad = recv_grad.reshape(slots, width)
    rows_gate = recv_gate.reshape(slots)
    w_first = w_in[0]
    w_second = w_out[0]
    hidden = jnp.dot(rows_in, w_first, preferred_element_type=jnp.float32)
    active, pullback = jax.vjp(gelu_tanh, hidden)
    active_low = lax.optimization_barrier(active.astype(jnp.bfloat16))
    gate_col = rows_gate.astype(jnp.float32)[:, None]
    scaled_grad = (gate_col * rows_grad.astype(jnp.float32)).astype(jnp.bfloat16)
    second_low = jnp.dot(
        active_low.T, scaled_grad, preferred_element_type=jnp.float32
    ).astype(jnp.bfloat16)
    second_low, rows_grad = lax.optimization_barrier((second_low, rows_grad))
    second_part = lax.psum_scatter(second_low, "dp", scatter_dimension=0, tiled=True)
    back_proj = jnp.dot(rows_grad, w_second.T, preferred_element_type=jnp.float32)
    gate_terms = jnp.sum(back_proj * active_low.astype(jnp.float32), axis=-1)
    hidden_grad = pullback(gate_col * back_proj)[0].astype(jnp.bfloat16)
    first_low = jnp.dot(
        rows_in.T, hidden_grad, preferred_element_type=jnp.float32
    ).astype(jnp.bfloat16)
    first_low, hidden_grad, gate_terms, stat_sums = lax.optimization_barrier(
        (first_low, hidden_grad, gate_terms, stat_sums)
    )
    first_part = lax.psum_scatter(first_low, "dp", scatter_dimension=1, tiled=True)
    importance, load = lax.psum(stat_sums, ("expert", "dp"))
    rows_back = jnp.dot(hidden_grad, w_first.T, preferred_element_type=jnp.float32)
    back_rows = rows_back.astype(jnp.bfloat16).reshape(experts, capacity, width)
    back_gate = gate_terms.astype(jnp.bfloat16).reshape(experts, capacity)
    home_rows, home_gate = (
        lax.all_to_all(back_rows, "expert", split_axis=0, concat_axis=0, tiled=True),
        lax.all_to_all(back_gate, "expert", split_axis=0, concat_axis=0, tiled=True),
    )
    expert_back = jnp.dot(
        assign_tok.T, home_rows.reshape(slots, width), preferred_element_type=jnp.float32
    )
    gate_grad = jnp.dot(
        home_gate.reshape(slots), assign, preferred_element_type=jnp.float32
    ).reshape(tok_rows, 2)
    total_weight = aux_weight * total_tokens
    imp_coef = total_weight * spread_grad(importance)
    load_coef = total_weight * spread_grad(load)
    score_grad = jnp.sum(jnp.where(top_hot, gate_grad[:, :, None], 0.0), axis=1) + imp_coef[None, :]
    noisy_grad = probs * (score_grad - jnp.sum(probs * score_grad, axis=-1, keepdims=True))
    z_grad = load_coef[None, :] * inv_root_tau * jnp.exp(-0.5 * zscore * zscore)
    logit_grad = (
        noisy_grad
        + z_grad / noise_std
        - jnp.where(thresh_hot, jnp.sum(z_grad, axis=-1, keepdims=True) / noise_std, 0.0)
    )
    logit_low = logit_grad.astype(jnp.bfloat16)
    router_back = jnp.dot(logit_low, router_weight.T, preferred_element_type=jnp.float32)
    patch_grad = (expert_back + router_back).astype(jnp.bfloat16)
    weight_part = jnp.dot(patches.T, logit_low, preferred_element_type=jnp.float32)
    router_weight_grad, router_bias_grad = lax.psum(
        (weight_part, jnp.sum(logit_grad, axis=0)), ("expert", "dp")
    )
    return (
        patch_grad,
        first_part[None],
        second_part[None],
        router_weight_grad,
        router_bias_grad,
    )


def solution(mesh):
    placed = (
        P(("expert", "dp"), None),
        P(),
        P(),
        P(("expert", "dp"), None),
        P(("expert", "dp"), None),
        P(("expert", "dp")),
        P("expert", None, None),
        P("expert", None, None),
        P(("expert", "dp"), None),
    )
    return jax.shard_map(
        on_device,
        mesh=mesh,
        in_specs=placed,
        out_specs=(
            P(("expert", "dp"), None),
            P("expert", None, "dp"),
            P("expert", "dp", None),
            P(),
            P(),
        ),
        check_vma=False,
    )
```

```python
import jax
import jax.numpy as jnp
from jax import lax
from jax.sharding import PartitionSpec as P


noise_std = 1.0
aux_weight = 1.0
inv_root_two = 0.7071067811865476
inv_root_tau = 0.3989422804014327


def gelu_tanh(values):
    return jax.nn.gelu(values, approximate=True)


def spread_grad(values):
    number = values.shape[0]
    average = jnp.mean(values)
    spread = jnp.mean((values - average) ** 2)
    return (2.0 * (values - average) - 2.0 * spread / average) / (number * average * average)


def on_device(
    patches, router_weight, router_bias, noise, top_experts, threshold_expert, w_in, w_out, out_grad
):
    tok_rows = patches.shape[0]
    width = patches.shape[1]
    experts = router_weight.shape[1]
    capacity = 5 * tok_rows // (2 * experts)
    slots = experts * capacity
    total_tokens = tok_rows * lax.axis_size("expert") * lax.axis_size("dp")
    logits = jnp.dot(patches, router_weight, preferred_element_type=jnp.float32) + router_bias
    noisy = logits + noise_std * noise
    probs = jax.nn.softmax(noisy, axis=-1)
    expert_ids = lax.broadcasted_iota(jnp.int32, (1, experts), 1)
    thresh_hot = threshold_expert[:, None] == expert_ids
    base = jnp.sum(jnp.where(thresh_hot, noisy, 0.0), axis=-1, keepdims=True)
    zscore = (logits - base) / noise_std
    stat_sums = (
        jnp.sum(probs, axis=0),
        jnp.sum(0.5 * (1.0 + lax.erf(zscore * inv_root_two)), axis=0),
    )
    top_hot = top_experts[:, :, None] == expert_ids[None]
    gates = jnp.sum(jnp.where(top_hot, probs[:, None, :], 0.0), axis=-1).astype(jnp.bfloat16)
    flat = top_experts.reshape(-1)
    flat_hot = (flat[:, None] == expert_ids).astype(jnp.int32)
    before = jnp.sum((jnp.cumsum(flat_hot, axis=0) - flat_hot) * flat_hot, axis=-1)
    slot_ids = flat * capacity + before
    slot_index = lax.broadcasted_iota(jnp.int32, (slots, 1), 0)
    assign = (slot_index == slot_ids[None, :]).astype(jnp.bfloat16)
    assign_tok = jnp.sum(assign.reshape(slots, tok_rows, 2), axis=-1)
    sent_in = (
        jnp.dot(assign_tok, patches, preferred_element_type=jnp.float32)
        .astype(jnp.bfloat16)
        .reshape(experts, capacity, width)
    )
    sent_grad = (
        jnp.dot(assign_tok, out_grad, preferred_element_type=jnp.float32)
        .astype(jnp.bfloat16)
        .reshape(experts, capacity, width)
    )
    sent_gate = (
        jnp.dot(assign, gates.reshape(-1), preferred_element_type=jnp.float32)
        .astype(jnp.bfloat16)
        .reshape(experts, capacity)
    )
    recv_in = lax.all_to_all(sent_in, "expert", split_axis=0, concat_axis=0, tiled=True)
    recv_grad = lax.all_to_all(sent_grad, "expert", split_axis=0, concat_axis=0, tiled=True)
    recv_gate = lax.all_to_all(sent_gate, "expert", split_axis=0, concat_axis=0, tiled=True)
    rows_in = recv_in.reshape(slots, width)
    rows_grad = recv_grad.reshape(slots, width)
    rows_gate = recv_gate.reshape(slots)
    w_first = w_in[0]
    w_second = w_out[0]
    hidden = jnp.dot(rows_in, w_first, preferred_element_type=jnp.float32)
    active, pullback = jax.vjp(gelu_tanh, hidden)
    active_low = lax.optimization_barrier(active.astype(jnp.bfloat16))
    gate_col = rows_gate.astype(jnp.float32)[:, None]
    scaled_grad = (gate_col * rows_grad.astype(jnp.float32)).astype(jnp.bfloat16)
    second_low = jnp.dot(
        active_low.T, scaled_grad, preferred_element_type=jnp.float32
    ).astype(jnp.bfloat16)
    second_low, rows_grad = lax.optimization_barrier((second_low, rows_grad))
    second_part = lax.psum_scatter(second_low, "dp", scatter_dimension=0, tiled=True)
    back_proj = jnp.dot(rows_grad, w_second.T, preferred_element_type=jnp.float32)
    gate_terms = jnp.sum(back_proj * active_low.astype(jnp.float32), axis=-1)
    hidden_grad = pullback(gate_col * back_proj)[0].astype(jnp.bfloat16)
    first_low = jnp.dot(
        rows_in.T, hidden_grad, preferred_element_type=jnp.float32
    ).astype(jnp.bfloat16)
    first_low, hidden_grad, gate_terms, stat_sums = lax.optimization_barrier(
        (first_low, hidden_grad, gate_terms, stat_sums)
    )
    first_part = lax.psum_scatter(first_low, "dp", scatter_dimension=1, tiled=True)
    importance, load = lax.psum(stat_sums, ("expert", "dp"))
    rows_back = jnp.dot(hidden_grad, w_first.T, preferred_element_type=jnp.float32)
    back_rows = rows_back.astype(jnp.bfloat16).reshape(experts, capacity, width)
    back_gate = gate_terms.astype(jnp.bfloat16).reshape(experts, capacity)
    home_rows, home_gate = (
        lax.all_to_all(back_rows, "expert", split_axis=0, concat_axis=0, tiled=True),
        lax.all_to_all(back_gate, "expert", split_axis=0, concat_axis=0, tiled=True),
    )
    expert_back = jnp.dot(
        assign_tok.T, home_rows.reshape(slots, width), preferred_element_type=jnp.float32
    )
    gate_grad = jnp.dot(
        home_gate.reshape(slots), assign, preferred_element_type=jnp.float32
    ).reshape(tok_rows, 2)
    total_weight = aux_weight * total_tokens
    imp_coef = total_weight * spread_grad(importance)
    load_coef = total_weight * spread_grad(load)
    score_grad = jnp.sum(jnp.where(top_hot, gate_grad[:, :, None], 0.0), axis=1) + imp_coef[None, :]
    noisy_grad = probs * (score_grad - jnp.sum(probs * score_grad, axis=-1, keepdims=True))
    z_grad = load_coef[None, :] * inv_root_tau * jnp.exp(-0.5 * zscore * zscore)
    logit_grad = (
        noisy_grad
        + z_grad / noise_std
        - jnp.where(thresh_hot, jnp.sum(z_grad, axis=-1, keepdims=True) / noise_std, 0.0)
    )
    logit_low = logit_grad.astype(jnp.bfloat16)
    router_back = jnp.dot(logit_low, router_weight.T, preferred_element_type=jnp.float32)
    patch_grad = (expert_back + router_back).astype(jnp.bfloat16)
    weight_part = jnp.dot(patches.T, logit_low, preferred_element_type=jnp.float32)
    router_weight_grad, router_bias_grad = lax.psum(
        (weight_part, jnp.sum(logit_grad, axis=0)), ("expert", "dp")
    )
    return (
        patch_grad,
        first_part[None],
        second_part[None],
        router_weight_grad,
        router_bias_grad,
    )


def solution(mesh):
    placed = (
        P(("expert", "dp"), None),
        P(),
        P(),
        P(("expert", "dp"), None),
        P(("expert", "dp"), None),
        P(("expert", "dp")),
        P("expert", None, None),
        P("expert", None, None),
        P(("expert", "dp"), None),
    )
    return jax.shard_map(
        on_device,
        mesh=mesh,
        in_specs=placed,
        out_specs=(
            P(("expert", "dp"), None),
            P("expert", None, "dp"),
            P("expert", "dp", None),
            P(),
            P(),
        ),
        check_vma=False,
    )
```
